32 devices in a mesh: dp: 2 (over x), hp: 4 (over z), cp: 4 (over y, core).
Axes of the slice: x: 2, y: 2, z: 4, core: 2. Of those that a mesh axis runs over, the one named last changes fastest.
Arguments:
- latent: bfloat16 [256, 16, 96, 128], P(('dp', 'cp'), 'hp'), parts along dimension 0
- conv_w: bfloat16 [4, 3, 3, 3, 128, 128], replicated
- conv_b: float32 [4, 128], replicated
- gn_gamma: float32 [4, 128], replicated
- gn_beta: float32 [4, 128], replicated
Outputs:
- output: bfloat16 [256, 16, 96, 128], P(('dp', 'cp'), 'hp'), parts along dimension 0
There are 2 independent parts. The reference program is written for one: setup_inputs(seed, part) draws one part's arguments, and reference() takes and returns one part's arrays. A program takes and returns all parts, laid end to end along the dimension named above; an argument that names none is the same for every part.
All inputs are finite; a program needn't handle non-finite values.
Results may differ from the reference program's by a relative error of at most 0.00957576.
Values are sent between devices in bfloat16 or wider.
A program may use at most 1 GiB of HBM per device.

```python
import jax
import jax.numpy as jnp
from jax import lax

FRAMES = 128
HEIGHT = 16
LAT_WIDTH = 96
CHANNELS = 128
GROUPS = 32
EPS = 1e-6


def setup_inputs(seed: int = 0, part: int = 0) -> dict:
    root_key = jax.random.key(seed)
    part_key = jax.random.fold_in(root_key, part)
    key_noise, key_fscale, key_fshift, key_rscale = jax.random.split(part_key, 4)
    key_kernel, key_bias, key_gamma, key_beta = jax.random.split(jax.random.key(seed + 1), 4)
    base_noise = jax.random.normal(key_noise, (FRAMES, HEIGHT, LAT_WIDTH, CHANNELS), jnp.float32)
    frame_scale = jnp.exp(0.5 * jax.random.normal(key_fscale, (FRAMES, 1, 1, 1), jnp.float32))
    frame_shift = 0.7 * jax.random.normal(key_fshift, (FRAMES, 1, 1, CHANNELS), jnp.float32)
    row_scale = jnp.exp(0.4 * jax.random.normal(key_rscale, (1, HEIGHT, 1, 1), jnp.float32))
    latent = ((base_noise + frame_shift) * frame_scale * row_scale).astype(jnp.bfloat16)
    fan_in = 27 * CHANNELS
    conv_w = (jax.random.normal(key_kernel, (4, 3, 3, 3, CHANNELS, CHANNELS), jnp.float32) * fan_in ** -0.5).astype(jnp.bfloat16)
    conv_b = 0.5 * jax.random.normal(key_bias, (4, CHANNELS), jnp.float32)
    gn_gamma = 1.0 + 0.3 * jax.random.normal(key_gamma, (4, CHANNELS), jnp.float32)
    gn_beta = 0.3 * jax.random.normal(key_beta, (4, CHANNELS), jnp.float32)
    return {"latent": latent, "conv_w": conv_w, "conv_b": conv_b, "gn_gamma": gn_gamma, "gn_beta": gn_beta}


def norm_silu(video, gamma, beta):
    per_group = CHANNELS // GROUPS
    grouped = video.reshape(FRAMES, HEIGHT, LAT_WIDTH, GROUPS, per_group).astype(jnp.float32)
    norm_count = FRAMES * HEIGHT * LAT_WIDTH * per_group
    mean_val = jnp.sum(grouped, axis=(0, 1, 2, 4)) / norm_count
    variance = jnp.sum(grouped * grouped, axis=(0, 1, 2, 4)) / norm_count - mean_val * mean_val
    inv_std = lax.rsqrt(variance + EPS)
    gamma_g = gamma.reshape(GROUPS, per_group)
    scale_c = (inv_std[:, None] * gamma_g).reshape(CHANNELS)
    shift_c = (beta.reshape(GROUPS, per_group) - (mean_val * inv_std)[:, None] * gamma_g).reshape(CHANNELS)
    return jax.nn.silu(video.astype(jnp.float32) * scale_c + shift_c).astype(jnp.bfloat16)


def causal_conv(video, kernel, bias_vec):
    padded = jnp.concatenate([video[:1], video[:1], video], axis=0)
    kernel_f = kernel.astype(jnp.float32)

    def one_frame(frame_idx):
        window = lax.dynamic_slice_in_dim(padded, frame_idx, 3, axis=0).astype(jnp.float32)
        conv_out = lax.conv_general_dilated(window[None], kernel_f, (1, 1, 1), ((0, 0), (1, 1), (1, 1)), dimension_numbers=("NDHWC", "DHWIO", "NDHWC"))
        return (conv_out[0, 0] + bias_vec).astype(jnp.bfloat16)

    return lax.map(one_frame, jnp.arange(FRAMES))


def reference(latent, conv_w, conv_b, gn_gamma, gn_beta):
    residual = latent
    for block_idx in range(2):
        hidden = residual
        for sub_idx in range(2):
            layer_idx = 2 * block_idx + sub_idx
            activated = norm_silu(hidden, gn_gamma[layer_idx], gn_beta[layer_idx])
            hidden = causal_conv(activated, conv_w[layer_idx], conv_b[layer_idx])
        residual = (residual.astype(jnp.float32) + hidden.astype(jnp.float32)).astype(jnp.bfloat16)
    return residual
```

```python
import functools

import jax
import jax.numpy as jnp
from jax import lax
from jax.experimental import pallas as pl
from jax.experimental.pallas import tpu as pltpu
from jax.sharding import PartitionSpec as P

GROUPS = 32
EPS = 1e-6
CHUNK = 4
MESH = pl.DeviceIdType.MESH
F32 = jnp.float32
BF16 = jnp.bfloat16


def group_sum(v, lane):
    n = v.shape[-1]
    v = v + jnp.where(lane % 2 == 0, pltpu.roll(v, n - 1, 1), pltpu.roll(v, 1, 1))
    return v + jnp.where(lane % 4 < 2, pltpu.roll(v, n - 2, 1), pltpu.roll(v, 2, 1))


def kernel(cfg, lat_ref, w_ref, bias_ref, gamma_ref, beta_ref, out_ref, raw_a, raw_b, act_a, act_b, w2_a, w2_b, stat,
           in_sem, out_sem, w_sem, row_send, row_recv, cp_send, cp_recv, st_send, st_recv):
    n_h, n_c, frames, rows, width, ch, total = cfg
    n_q = frames // CHUNK
    n_dev = n_h * n_c
    h = lax.axis_index("hp")
    c = lax.axis_index("cp")
    me = h * n_c + c
    has_up, has_down = h > 0, h < n_h - 1
    has_prev, has_next = c > 0, c < n_c - 1

    def device(idx):
        return {"hp": idx // n_c, "cp": lax.rem(idx, n_c)}

    barrier = pltpu.get_barrier_semaphore()
    for d in range(1, n_dev):
        pl.semaphore_signal(barrier, inc=1, device_id=device(lax.rem(me + d, n_dev)), device_id_type=MESH)

    def in_copy(k):
        return pltpu.make_async_copy(lat_ref.at[pl.ds(k * CHUNK, CHUNK)],
                                     raw_a.at[pl.ds(k * CHUNK + 2, CHUNK), 1:rows + 1], in_sem.at[k])

    for k in range(n_q):
        in_copy(k).start()

    def w_copies(layer, buf, which):
        return [pltpu.make_async_copy(w_ref.at[layer], buf.at[o:o + 3, :, :, :, o * ch:(o + 1) * ch], w_sem.at[which, o])
                for o in range(2)]

    for which, buf in enumerate((w2_a, w2_b)):
        for o in range(2):
            for i in range(3):
                for j in range(3):
                    buf[3 - 3 * o, i, j, :, o * ch:(o + 1) * ch] = jnp.zeros((ch, ch), BF16)
        for cp in w_copies(which, buf, which):
            cp.start()

    pl.semaphore_wait(barrier, n_dev - 1)

    raws = (raw_a, raw_b)

    def row_copy(k, buf, up, src=None):
        row = 0 if up else rows - 1
        fr = pl.ds(k * CHUNK + 2, CHUNK)
        source = raws[buf].at[fr, row + 1] if src is None else src.at[pl.ds(k * CHUNK, CHUNK), row]
        d = 0 if up else 1
        return pltpu.make_async_remote_copy(
            src_ref=source, dst_ref=raws[buf].at[fr, rows + 1 if up else 0],
            send_sem=row_send.at[buf, d, k], recv_sem=row_recv.at[buf, d, k],
            device_id={"hp": h - 1 if up else h + 1}, device_id_type=MESH)

    def row_start(k, buf, src=None):
        @pl.when(has_up)
        def _():
            row_copy(k, buf, True, src).start()

        @pl.when(has_down)
        def _():
            row_copy(k, buf, False, src).start()

    def row_wait(k, buf):
        @pl.when(has_down)
        def _():
            row_copy(k, buf, True).wait_recv()
            row_copy(k, buf, False).wait_send()

        @pl.when(has_up)
        def _():
            row_copy(k, buf, False).wait_recv()
            row_copy(k, buf, True).wait_send()

    def cp_copy(buf, part, src=None):
        lo, hi, dst_lo, dst_hi, dh = ((0, rows, 1, rows + 1, 0), (0, 1, rows + 1, rows + 2, -1),
                                      (rows - 1, rows, 0, 1, 1))[part]
        source = raws[buf].at[frames:frames + 2, lo + 1:hi + 1] if src is None else src.at[frames - 2:frames, lo:hi]
        return pltpu.make_async_remote_copy(
            src_ref=source, dst_ref=raws[buf].at[0:2, dst_lo:dst_hi],
            send_sem=cp_send.at[buf, part], recv_sem=cp_recv.at[buf, part],
            device_id={"hp": h + dh, "cp": c + 1}, device_id_type=MESH)

    def cp_start(buf, src=None):
        for part, cond in enumerate((has_next, has_next & has_up, has_next & has_down)):
            @pl.when(cond)
            def _():
                cp_copy(buf, part, src).start()

    def cp_wait(buf):
        for part, cond in enumerate((has_prev, has_prev & has_down, has_prev & has_up)):
            @pl.when(cond)
            def _():
                cp_copy(buf, part).wait_recv()
        for part, cond in enumerate((has_next, has_next & has_up, has_next & has_down)):
            @pl.when(cond)
            def _():
                cp_copy(buf, part).wait_send()

    def stat_copy(layer, d):
        return pltpu.make_async_remote_copy(
            src_ref=stat.at[layer, me], dst_ref=stat.at[layer, me],
            send_sem=st_send.at[layer, d], recv_sem=st_recv.at[layer, me],
            device_id=device(lax.rem(me + d, n_dev)), device_id_type=MESH)

    def stat_start(layer, s1, s2):
        stat[layer, me, 0:1, :] = jnp.sum(s1, axis=0, keepdims=True)
        stat[layer, me, 1:2, :] = jnp.sum(s2, axis=0, keepdims=True)
        for d in range(1, n_dev):
            stat_copy(layer, d).start()

    def stat_finish(layer):
        for d in range(1, n_dev):
            src = lax.rem(me + d, n_dev)
            pltpu.make_async_remote_copy(
                src_ref=stat.at[layer, src], dst_ref=stat.at[layer, src],
                send_sem=st_send.at[layer, d], recv_sem=st_recv.at[layer, src],
                device_id=device(src), device_id_type=MESH).wait_recv()
            stat_copy(layer, d).wait_send()
        lane = lax.broadcasted_iota(jnp.int32, (8, ch), 1)
        sums = jnp.sum(stat[layer], axis=0)
        s1 = group_sum(jnp.broadcast_to(sums[0:1], (8, ch)), lane)
        s2 = group_sum(jnp.broadcast_to(sums[1:2], (8, ch)), lane)
        mean = s1 / total
        inv = lax.rsqrt(s2 / total - mean * mean + EPS)
        scale = gamma_ref[pl.ds(layer, 1)] * inv
        shift = beta_ref[pl.ds(layer, 1)] - mean * scale
        return (0.5 * scale)[0:1], (0.5 * shift)[0:1]

    last = n_q - 1
    row_start(last, 0, lat_ref)
    row_start(last - 1, 0, lat_ref)

    def stats_of(v, s1, s2):
        v8 = v.reshape(v.shape[0] // 8, 8, ch)
        return s1 + jnp.sum(v8, axis=0), s2 + jnp.sum(v8 * v8, axis=0)

    zero = jnp.zeros((8, ch), F32)

    def x_stats(k, carry):
        in_copy(k).wait()
        s1, s2 = carry
        for f in range(CHUNK):
            for r in range(rows):
                s1, s2 = stats_of(raw_a[k * CHUNK + 2 + f, r + 1].astype(F32), s1, s2)
        return s1, s2

    stat_start(0, *lax.fori_loop(0, n_q, x_stats, (zero, zero)))
    for k in range(last - 2, -1, -1):
        row_start(k, 0, lat_ref)
    cp_start(0, lat_ref)

    sub = lax.broadcasted_iota(jnp.int32, (width, ch), 0)

    def norm_row(raw, frame, r, act, slot, scale, shift):
        t = raw[frame, r].astype(F32) * scale + shift
        v = t + t * jnp.tanh(t)
        if r == 0:
            v = jnp.where(has_up, v, 0.0)
        if r == rows + 1:
            v = jnp.where(has_down, v, 0.0)
        act[slot, r, :, 0:ch] = jnp.where(sub == 0, 0.0, pltpu.roll(v, 1, 0)).astype(BF16)
        act[slot, r, :, ch:2 * ch] = v.astype(BF16)
        act[slot, r, :, 2 * ch:3 * ch] = jnp.where(sub == width - 1, 0.0, pltpu.roll(v, width - 1, 0)).astype(BF16)

    first_frame = jnp.where(has_prev, 0, 2)

    def step(q, block, sub_idx, scale, shift, carry):
        src, dst = raws[sub_idx], raws[1 - sub_idx]
        parity = sub_idx
        act, nxt = (act_a, act_b) if step.even else (act_b, act_a)
        w2 = (w2_a, w2_b)[sub_idx]
        layer = 2 * block + sub_idx
        lhs = []
        for p in range(2):
            lhs.append(jnp.concatenate(
                [act[2 * p + k, i:i + rows].reshape(rows * width, 3 * ch) for k in range(4) for i in range(3)], axis=1))
        wmat = w2[...].reshape(36 * ch, 2 * ch)
        acc = jnp.dot(jnp.concatenate(lhs, axis=0), wmat, preferred_element_type=F32)
        base = jnp.maximum(q * CHUNK - CHUNK, 0)
        for f in range(CHUNK):
            frame = base + f if f >= 2 else jnp.maximum(base + f, first_frame)
            for r in range(rows + 2):
                norm_row(src, frame, r, nxt, f, scale, shift)
        nxt[CHUNK:CHUNK + 2] = act[0:2]
        s1, s2 = carry
        bias = bias_ref[pl.ds(layer, 1)]
        for p in range(2):
            for i in range(rows):
                for o in range(2):
                    at = (p * rows + i) * width
                    y = (acc[at:at + width, o * ch:(o + 1) * ch] + bias).astype(BF16)
                    frame = q * CHUNK + 2 + 2 * p + o
                    if sub_idx == 1:
                        y = (dst[frame, i + 1].astype(F32) + y.astype(F32)).astype(BF16)
                    dst[frame, i + 1] = y
                    s1, s2 = stats_of(y.astype(F32), s1, s2)
        return s1, s2

    def conv_layer(block, sub_idx, scale, shift):
        src = raws[sub_idx]
        for which in range(2):
            w_copies(sub_idx, (w2_a, w2_b)[sub_idx], sub_idx)[which].wait()
        row_wait(last, sub_idx)
        row_wait(last - 1, sub_idx)
        for f in range(CHUNK + 2):
            for r in range(rows + 2):
                norm_row(src, frames - CHUNK + f, r, act_a, f, scale, shift)

        def after(q):
            if sub_idx == 0:
                row_start(q, 1)
            else:
                @pl.when(block == 0)
                def _():
                    row_start(q, 0)

                @pl.when(block == 1)
                def _():
                    out_copy(q).start()

        def pair(i, carry):
            q = last - 2 * i

            @pl.when(i < n_q // 2 - 1)
            def _():
                row_wait(q - 2, sub_idx)

            @pl.when(i == n_q // 2 - 1)
            def _():
                cp_wait(sub_idx)

            step.even = True
            carry = step(q, block, sub_idx, scale, shift, carry)
            after(q)

            @pl.when(i == 0)
            def _():
                if sub_idx == 0:
                    cp_start(1)
                else:
                    @pl.when(block == 0)
                    def _():
                        cp_start(0)

            @pl.when(i < n_q // 2 - 1)
            def _():
                row_wait(q - 3, sub_idx)

            step.even = False
            carry = step(q - 1, block, sub_idx, scale, shift, carry)
            after(q - 1)
            return carry

        return lax.fori_loop(0, n_q // 2, pair, (zero, zero))

    def out_copy(q):
        return pltpu.make_async_copy(raw_a.at[pl.ds(q * CHUNK + 2, CHUNK), 1:rows + 1],
                                     out_ref.at[pl.ds(q * CHUNK, CHUNK)], out_sem.at[q])

    def block_body(block, _):
        scale, shift = stat_finish(2 * block)
        sums = conv_layer(block, 0, scale, shift)
        stat_start(2 * block + 1, *sums)

        @pl.when(block == 0)
        def _():
            for cp in w_copies(2, w2_a, 0):
                cp.start()

        scale, shift = stat_finish(2 * block + 1)
        sums = conv_layer(block, 1, scale, shift)

        @pl.when(block == 0)
        def _():
            stat_start(2, *sums)
            for cp in w_copies(3, w2_b, 1):
                cp.start()

        return 0

    lax.fori_loop(0, 2, block_body, 0)
    for q in range(n_q):
        out_copy(q).wait()


def solution(mesh):
    n_h, n_c = mesh.shape["hp"], mesh.shape["cp"]

    def local_decode(lat, conv_w, conv_b, gamma, beta):
        frames, rows, width, ch = lat.shape
        total = float(frames * n_c * rows * n_h * width * (ch // GROUPS))
        n_q = frames // CHUNK
        cfg = (n_h, n_c, frames, rows, width, ch, total)
        vmem = pl.BlockSpec(memory_space=pltpu.VMEM)
        anym = pl.BlockSpec(memory_space=pl.ANY)
        dma = pltpu.SemaphoreType.DMA
        return pl.pallas_call(
            functools.partial(kernel, cfg),
            out_shape=jax.ShapeDtypeStruct(lat.shape, lat.dtype),
            in_specs=[anym, anym, vmem, vmem, vmem],
            out_specs=anym,
            scratch_shapes=[
                pltpu.VMEM((frames + 2, rows + 2, width, ch), BF16),
                pltpu.VMEM((frames + 2, rows + 2, width, ch), BF16),
                pltpu.VMEM((CHUNK + 2, rows + 2, width, 3 * ch), BF16),
                pltpu.VMEM((CHUNK + 2, rows + 2, width, 3 * ch), BF16),
                pltpu.VMEM((4, 3, 3, ch, 2 * ch), BF16),
                pltpu.VMEM((4, 3, 3, ch, 2 * ch), BF16),
                pltpu.VMEM((4, n_h * n_c, 2, ch), F32),
                dma((n_q,)), dma((n_q,)), dma((2, 2)),
                dma((2, 2, n_q)), dma((2, 2, n_q)), dma((2, 3)), dma((2, 3)),
                dma((4, n_h * n_c)), dma((4, n_h * n_c)),
            ],
            compiler_params=pltpu.CompilerParams(collective_id=0, has_side_effects=True, vmem_limit_bytes=60 * 1024 * 1024),
        )(lat, conv_w, conv_b, gamma, beta)

    spec = P(("dp", "cp"), "hp", None, None)
    return jax.shard_map(local_decode, mesh=mesh, in_specs=(spec, P(), P(), P(), P()), out_specs=spec, check_vma=False)
```

```python
import functools

import jax
import jax.numpy as jnp
from jax import lax
from jax.experimental import pallas as pl
from jax.experimental.pallas import tpu as pltpu
from jax.sharding import PartitionSpec as P

GROUPS = 32
EPS = 1e-6
CHUNK = 4
PARTS = 6
MESH = pl.DeviceIdType.MESH
F32 = jnp.float32
BF16 = jnp.bfloat16


def group_sum(v, lane):
    n = v.shape[-1]
    v = v + jnp.where(lane % 2 == 0, pltpu.roll(v, n - 1, 1), pltpu.roll(v, 1, 1))
    return v + jnp.where(lane % 4 < 2, pltpu.roll(v, n - 2, 1), pltpu.roll(v, 2, 1))


def kernel(cfg, lat_ref, w_ref, bias_ref, gamma_ref, beta_ref, out_ref, raw_a, raw_b, act_a, act_b, w2_a, w2_b, acc_buf, stat,
           in_sem, out_sem, w_sem, row_send, row_recv, cp_send, cp_recv, st_send, st_recv):
    n_h, n_c, frames, rows, width, ch, total = cfg
    n_q = frames // CHUNK
    n_dev = n_h * n_c
    h = lax.axis_index("hp")
    c = lax.axis_index("cp")
    me = h * n_c + c
    has_up, has_down = h > 0, h < n_h - 1
    has_prev, has_next = c > 0, c < n_c - 1

    def device(idx):
        return {"hp": idx // n_c, "cp": lax.rem(idx, n_c)}

    barrier = pltpu.get_barrier_semaphore()
    for d in range(1, n_dev):
        pl.semaphore_signal(barrier, inc=1, device_id=device(lax.rem(me + d, n_dev)), device_id_type=MESH)

    def in_copy(k):
        return pltpu.make_async_copy(lat_ref.at[pl.ds(k * CHUNK, CHUNK)],
                                     raw_a.at[pl.ds(k * CHUNK + 2, CHUNK), 1:rows + 1], in_sem.at[k])

    for k in range(n_q):
        in_copy(k).start()

    def w_copies(layer, buf, which):
        return [pltpu.make_async_copy(w_ref.at[layer], buf.at[o:o + 3, :, :, :, o * ch:(o + 1) * ch], w_sem.at[which, o])
                for o in range(2)]

    for which, buf in enumerate((w2_a, w2_b)):
        for o in range(2):
            for i in range(3):
                for j in range(3):
                    buf[3 - 3 * o, i, j, :, o * ch:(o + 1) * ch] = jnp.zeros((ch, ch), BF16)
        for cp in w_copies(which, buf, which):
            cp.start()

    pl.semaphore_wait(barrier, n_dev - 1)

    raws = (raw_a, raw_b)

    def row_copy(k, buf, up, src=None):
        row = 0 if up else rows - 1
        fr = pl.ds(k * CHUNK + 2, CHUNK)
        source = raws[buf].at[fr, row + 1] if src is None else src.at[pl.ds(k * CHUNK, CHUNK), row]
        d = 0 if up else 1
        return pltpu.make_async_remote_copy(
            src_ref=source, dst_ref=raws[buf].at[fr, rows + 1 if up else 0],
            send_sem=row_send.at[buf, d, k], recv_sem=row_recv.at[buf, d, k],
            device_id={"hp": h - 1 if up else h + 1}, device_id_type=MESH)

    def row_start(k, buf, src=None):
        @pl.when(has_up)
        def _():
            row_copy(k, buf, True, src).start()

        @pl.when(has_down)
        def _():
            row_copy(k, buf, False, src).start()

    def row_wait(k, buf):
        @pl.when(has_down)
        def _():
            row_copy(k, buf, True).wait_recv()
            row_copy(k, buf, False).wait_send()

        @pl.when(has_up)
        def _():
            row_copy(k, buf, False).wait_recv()
            row_copy(k, buf, True).wait_send()

    def cp_copy(buf, part, src=None):
        lo, hi, dst_lo, dst_hi, dh = ((0, rows, 1, rows + 1, 0), (0, 1, rows + 1, rows + 2, -1),
                                      (rows - 1, rows, 0, 1, 1))[part]
        source = raws[buf].at[frames:frames + 2, lo + 1:hi + 1] if src is None else src.at[frames - 2:frames, lo:hi]
        return pltpu.make_async_remote_copy(
            src_ref=source, dst_ref=raws[buf].at[0:2, dst_lo:dst_hi],
            send_sem=cp_send.at[buf, part], recv_sem=cp_recv.at[buf, part],
            device_id={"hp": h + dh, "cp": c + 1}, device_id_type=MESH)

    def cp_start(buf, src=None):
        for part, cond in enumerate((has_next, has_next & has_up, has_next & has_down)):
            @pl.when(cond)
            def _():
                cp_copy(buf, part, src).start()

    def cp_wait(buf):
        for part, cond in enumerate((has_prev, has_prev & has_down, has_prev & has_up)):
            @pl.when(cond)
            def _():
                cp_copy(buf, part).wait_recv()
        for part, cond in enumerate((has_next, has_next & has_up, has_next & has_down)):
            @pl.when(cond)
            def _():
                cp_copy(buf, part).wait_send()

    def stat_copy(layer, d):
        return pltpu.make_async_remote_copy(
            src_ref=stat.at[layer, me], dst_ref=stat.at[layer, me],
            send_sem=st_send.at[layer, d], recv_sem=st_recv.at[layer, me],
            device_id=device(lax.rem(me + d, n_dev)), device_id_type=MESH)

    def stat_start(layer, s1, s2):
        stat[layer, me, 0:1, :] = jnp.sum(s1, axis=0, keepdims=True)
        stat[layer, me, 1:2, :] = jnp.sum(s2, axis=0, keepdims=True)
        for d in range(1, n_dev):
            stat_copy(layer, d).start()

    def stat_finish(layer):
        for d in range(1, n_dev):
            src = lax.rem(me + d, n_dev)
            pltpu.make_async_remote_copy(
                src_ref=stat.at[layer, src], dst_ref=stat.at[layer, src],
                send_sem=st_send.at[layer, d], recv_sem=st_recv.at[layer, src],
                device_id=device(src), device_id_type=MESH).wait_recv()
            stat_copy(layer, d).wait_send()
        lane = lax.broadcasted_iota(jnp.int32, (8, ch), 1)
        sums = jnp.sum(stat[layer], axis=0)
        s1 = group_sum(jnp.broadcast_to(sums[0:1], (8, ch)), lane)
        s2 = group_sum(jnp.broadcast_to(sums[1:2], (8, ch)), lane)
        mean = s1 / total
        inv = lax.rsqrt(s2 / total - mean * mean + EPS)
        scale = gamma_ref[pl.ds(layer, 1)] * inv
        shift = beta_ref[pl.ds(layer, 1)] - mean * scale
        return (0.5 * scale)[0:1], (0.5 * shift)[0:1]

    last = n_q - 1
    row_start(last, 0, lat_ref)
    row_start(last - 1, 0, lat_ref)

    def stats_of(v, s1, s2):
        v8 = v.reshape(v.shape[0] // 8, 8, ch)
        return s1 + jnp.sum(v8, axis=0), s2 + jnp.sum(v8 * v8, axis=0)

    zero = jnp.zeros((8, ch), F32)

    def x_stats(k, carry):
        in_copy(k).wait()
        s1, s2 = carry
        for f in range(CHUNK):
            for r in range(rows):
                s1, s2 = stats_of(raw_a[k * CHUNK + 2 + f, r + 1].astype(F32), s1, s2)
        return s1, s2

    stat_start(0, *lax.fori_loop(0, n_q, x_stats, (zero, zero)))
    for k in range(last - 2, -1, -1):
        row_start(k, 0, lat_ref)
    cp_start(0, lat_ref)

    sub = lax.broadcasted_iota(jnp.int32, (width, ch), 0)

    def norm_row(raw, frame, r, act, slot, scale, shift):
        t = raw[frame, r].astype(F32) * scale + shift
        v = t + t * jnp.tanh(t)
        if r == 0:
            v = jnp.where(has_up, v, 0.0)
        if r == rows + 1:
            v = jnp.where(has_down, v, 0.0)
        act[slot, r, :, 0:ch] = jnp.where(sub == 0, 0.0, pltpu.roll(v, 1, 0)).astype(BF16)
        act[slot, r, :, ch:2 * ch] = v.astype(BF16)
        act[slot, r, :, 2 * ch:3 * ch] = jnp.where(sub == width - 1, 0.0, pltpu.roll(v, width - 1, 0)).astype(BF16)

    first_frame = jnp.where(has_prev, 0, 2)

    def step(q, block, sub_idx, par, scale, shift, carry):
        src = raws[sub_idx]
        act, nxt = (act_a, act_b) if par == 0 else (act_b, act_a)
        w2 = (w2_a, w2_b)[sub_idx]
        base = jnp.maximum(q * CHUNK - CHUNK, 0)
        sums = [carry]

        def norm_item(f, r):
            frame = base + f if f >= 2 else jnp.maximum(base + f, first_frame)
            norm_row(src, frame, r, nxt, f, scale, shift)

        def tail_item(p, i):
            sums[0] = epilogue(q + 1, block, sub_idx, 1 - par, p, i, sums[0])

        norms = [functools.partial(norm_item, f, r) for f in range(CHUNK) for r in range(rows + 2)]
        tails = [functools.partial(tail_item, p, i) for i in range(rows) for p in range(2)]
        items = []
        for n in range(len(tails)):
            items += norms[3 * n:3 * n + 3] + [tails[n]]
        acc, done = [None, None], 0
        for kt in range(PARTS):
            weights = weight_part(w2, kt)
            for p in range(2):
                part = jnp.dot(lhs_part(act, p, kt), weights, preferred_element_type=F32)
                acc[p] = part if acc[p] is None else acc[p] + part
            upto = (kt + 1) * len(items) // PARTS
            for item in items[done:upto]:
                item()
            done = upto
        for p in range(2):
            acc_buf[par, p] = acc[p]
        nxt[CHUNK:CHUNK + 2] = act[0:2]
        return sums[0]

    def blocks(kt):
        n = 36 // PARTS
        return [divmod(b, 3) for b in range(kt * n, (kt + 1) * n)]

    def weight_part(w2, kt):
        return jnp.concatenate([w2[n // 3, n % 3, j] for n, j in blocks(kt)], axis=0)

    def lhs_part(act, p, kt):
        return jnp.concatenate([act[2 * p + n // 3, n % 3:n % 3 + rows, :, j * ch:(j + 1) * ch].reshape(rows * width, ch)
                                for n, j in blocks(kt)], axis=1)

    def epilogue(q, block, sub_idx, par, p, i, sums):
        dst = raws[1 - sub_idx]
        acc = acc_buf[par, p, i * width:(i + 1) * width]
        bias = bias_ref[pl.ds(2 * block + sub_idx, 1)]
        for o in range(2):
            y = (acc[:, o * ch:(o + 1) * ch] + bias).astype(BF16)
            frame = q * CHUNK + 2 + 2 * p + o
            if sub_idx == 1:
                y = (dst[frame, i + 1].astype(F32) + y.astype(F32)).astype(BF16)
            dst[frame, i + 1] = y
            sums = stats_of(y.astype(F32), *sums)
        return sums

    def conv_layer(block, sub_idx, scale, shift):
        src = raws[sub_idx]
        for cp in w_copies(sub_idx, (w2_a, w2_b)[sub_idx], sub_idx):
            cp.wait()
        row_wait(last, sub_idx)
        row_wait(last - 1, sub_idx)
        for f in range(CHUNK + 2):
            for r in range(rows + 2):
                norm_row(src, frames - CHUNK + f, r, act_a, f, scale, shift)

        def pair(i, carry):
            q = last - 2 * i

            @pl.when(i < n_q // 2 - 1)
            def _():
                row_wait(q - 2, sub_idx)

            @pl.when(i == n_q // 2 - 1)
            def _():
                cp_wait(sub_idx)

            s1, s2 = step(q, block, sub_idx, 0, scale, shift, carry)
            carry = jnp.where(i == 0, 0.0, s1), jnp.where(i == 0, 0.0, s2)

            @pl.when(i > 0)
            def _():
                after(q + 1, block, sub_idx)

            @pl.when(i < n_q // 2 - 1)
            def _():
                row_wait(q - 3, sub_idx)

            carry = step(q - 1, block, sub_idx, 1, scale, shift, carry)
            after(q, block, sub_idx)

            @pl.when(i == 0)
            def _():
                if sub_idx == 0:
                    cp_start(1)
                else:
                    @pl.when(block == 0)
                    def _():
                        cp_start(0)

            return carry

        sums = lax.fori_loop(0, n_q // 2, pair, (zero, zero))
        for i in range(rows):
            for p in range(2):
                sums = epilogue(0, block, sub_idx, 1, p, i, sums)
        return sums

    def after(q, block, sub_idx):
        if sub_idx == 0:
            row_start(q, 1)
        else:
            @pl.when(block == 0)
            def _():
                row_start(q, 0)

            @pl.when(block == 1)
            def _():
                out_copy(q).start()

    def out_copy(q):
        return pltpu.make_async_copy(raw_a.at[pl.ds(q * CHUNK + 2, CHUNK), 1:rows + 1],
                                     out_ref.at[pl.ds(q * CHUNK, CHUNK)], out_sem.at[q])

    def block_body(block, _):
        scale, shift = stat_finish(2 * block)
        sums = conv_layer(block, 0, scale, shift)
        stat_start(2 * block + 1, *sums)
        after(0, block, 0)

        @pl.when(block == 0)
        def _():
            for cp in w_copies(2, w2_a, 0):
                cp.start()

        scale, shift = stat_finish(2 * block + 1)
        sums = conv_layer(block, 1, scale, shift)

        @pl.when(block == 0)
        def _():
            stat_start(2, *sums)
            for cp in w_copies(3, w2_b, 1):
                cp.start()

        after(0, block, 1)
        return 0

    lax.fori_loop(0, 2, block_body, 0)
    for q in range(n_q):
        out_copy(q).wait()


def solution(mesh):
    n_h, n_c = mesh.shape["hp"], mesh.shape["cp"]

    def local_decode(lat, conv_w, conv_b, gamma, beta):
        frames, rows, width, ch = lat.shape
        total = float(frames * n_c * rows * n_h * width * (ch // GROUPS))
        n_q = frames // CHUNK
        cfg = (n_h, n_c, frames, rows, width, ch, total)
        vmem = pl.BlockSpec(memory_space=pltpu.VMEM)
        anym = pl.BlockSpec(memory_space=pl.ANY)
        dma = pltpu.SemaphoreType.DMA
        return pl.pallas_call(
            functools.partial(kernel, cfg),
            out_shape=jax.ShapeDtypeStruct(lat.shape, lat.dtype),
            in_specs=[anym, anym, vmem, vmem, vmem],
            out_specs=anym,
            scratch_shapes=[
                pltpu.VMEM((frames + 2 + CHUNK, rows + 2, width, ch), BF16),
                pltpu.VMEM((frames + 2 + CHUNK, rows + 2, width, ch), BF16),
                pltpu.VMEM((CHUNK + 2, rows + 2, width, 3 * ch), BF16),
                pltpu.VMEM((CHUNK + 2, rows + 2, width, 3 * ch), BF16),
                pltpu.VMEM((4, 3, 3, ch, 2 * ch), BF16),
                pltpu.VMEM((4, 3, 3, ch, 2 * ch), BF16),
                pltpu.VMEM((2, 2, rows * width, 2 * ch), F32),
                pltpu.VMEM((4, n_h * n_c, 2, ch), F32),
                dma((n_q,)), dma((n_q,)), dma((2, 2)),
                dma((2, 2, n_q)), dma((2, 2, n_q)), dma((2, 3)), dma((2, 3)),
                dma((4, n_h * n_c)), dma((4, n_h * n_c)),
            ],
            compiler_params=pltpu.CompilerParams(collective_id=0, has_side_effects=True, vmem_limit_bytes=60 * 1024 * 1024),
        )(lat, conv_w, conv_b, gamma, beta)

    spec = P(("dp", "cp"), "hp", None, None)
    return jax.shard_map(local_decode, mesh=mesh, in_specs=(spec, P(), P(), P(), P()), out_specs=spec, check_vma=False)
```

```python
import functools

import jax
import jax.numpy as jnp
from jax import lax
from jax.experimental import pallas as pl
from jax.experimental.pallas import tpu as pltpu
from jax.sharding import PartitionSpec as P

GROUPS = 32
EPS = 1e-6
CHUNK = 4
MESH = pl.DeviceIdType.MESH
F32 = jnp.float32
BF16 = jnp.bfloat16


def group_sum(v, lane):
    n = v.shape[-1]
    v = v + jnp.where(lane % 2 == 0, pltpu.roll(v, n - 1, 1), pltpu.roll(v, 1, 1))
    return v + jnp.where(lane % 4 < 2, pltpu.roll(v, n - 2, 1), pltpu.roll(v, 2, 1))


def kernel(cfg, lat_ref, w_ref, bias_ref, gamma_ref, beta_ref, out_ref, raw_a, raw_b, act_a, act_b, wa_a, wa_b, wb_a, wb_b, acc_t, acc_r, stat,
           in_sem, out_sem, w_sem, row_send, row_recv, cp_send, cp_recv, st_send, st_recv):
    n_h, n_c, frames, rows, width, ch, total = cfg
    n_q = frames // CHUNK
    n_dev = n_h * n_c
    h = lax.axis_index("hp")
    c = lax.axis_index("cp")
    me = h * n_c + c
    has_up, has_down = h > 0, h < n_h - 1
    has_prev, has_next = c > 0, c < n_c - 1

    def device(idx):
        return {"hp": idx // n_c, "cp": lax.rem(idx, n_c)}

    barrier = pltpu.get_barrier_semaphore()
    for d in range(1, n_dev):
        pl.semaphore_signal(barrier, inc=1, device_id=device(lax.rem(me + d, n_dev)), device_id_type=MESH)

    def in_copy(k):
        return pltpu.make_async_copy(lat_ref.at[pl.ds(k * CHUNK, CHUNK)],
                                     raw_a.at[pl.ds(k * CHUNK + 2, CHUNK), 1:rows + 1], in_sem.at[k])

    for k in range(n_q):
        in_copy(k).start()

    wts = ((wa_a, wb_a), (wa_b, wb_b))

    def w_copies(layer, which):
        wa, wb = wts[which]
        pairs = [(w_ref.at[layer, 1:3], wa.at[:, :, :, :, 0:ch]), (w_ref.at[layer, 0:2], wa.at[:, :, :, :, ch:2 * ch])]
        for o in range(2):
            for n in range(2):
                pairs.append((w_ref.at[layer, 2 * o], wb.at[o, n:n + 3, :, :, n * ch:(n + 1) * ch]))
        return [pltpu.make_async_copy(src, dst, w_sem.at[which, n]) for n, (src, dst) in enumerate(pairs)]

    for which in range(2):
        wb = wts[which][1]
        for o in range(2):
            for j in range(3):
                for n in range(2):
                    wb[o, 3 - 3 * n, j, :, n * ch:(n + 1) * ch] = jnp.zeros((ch, ch), BF16)
        for cp in w_copies(which, which):
            cp.start()

    raws = (raw_a, raw_b)

    def row_copy(k, buf, up):
        fr = {0: pl.ds(2, CHUNK - 2), n_q: pl.ds(frames, 2)}.get(k, pl.ds(k * CHUNK, CHUNK)) if isinstance(k, int) else pl.ds(k * CHUNK, CHUNK)
        d = 0 if up else 1
        return pltpu.make_async_remote_copy(
            src_ref=raws[buf].at[fr, 1 if up else rows], dst_ref=raws[buf].at[fr, rows + 1 if up else 0],
            send_sem=row_send.at[buf, d, k], recv_sem=row_recv.at[buf, d, k],
            device_id={"hp": h - 1 if up else h + 1}, device_id_type=MESH)

    def rows_start(chunks, buf):
        for up, cond in ((True, has_up), (False, has_down)):
            @pl.when(cond)
            def _():
                for k in chunks:
                    row_copy(k, buf, up).start()

    def rows_wait(chunks, buf):
        for up, cond in ((True, has_down), (False, has_up)):
            @pl.when(cond)
            def _():
                for k in chunks:
                    row_copy(k, buf, up).wait_recv()
                    row_copy(k, buf, not up).wait_send()

    def cp_copy(buf, part, src=None):
        lo, hi, dst_lo, dst_hi, dh = ((0, rows, 1, rows + 1, 0), (0, 1, rows + 1, rows + 2, -1),
                                      (rows - 1, rows, 0, 1, 1))[part]
        source = raws[buf].at[frames:frames + 2, lo + 1:hi + 1] if src is None else src.at[frames - 2:frames, lo:hi]
        return pltpu.make_async_remote_copy(
            src_ref=source, dst_ref=raws[buf].at[0:2, dst_lo:dst_hi],
            send_sem=cp_send.at[buf, part], recv_sem=cp_recv.at[buf, part],
            device_id={"hp": h + dh, "cp": c + 1}, device_id_type=MESH)

    def cp_start(buf, src=None):
        for part, cond in enumerate((has_next, has_next & has_up, has_next & has_down)):
            @pl.when(cond)
            def _():
                cp_copy(buf, part, src).start()

    def cp_wait(buf):
        for part, cond in enumerate((has_prev, has_prev & has_down, has_prev & has_up)):
            @pl.when(cond)
            def _():
                cp_copy(buf, part).wait_recv()
        for part, cond in enumerate((has_next, has_next & has_up, has_next & has_down)):
            @pl.when(cond)
            def _():
                cp_copy(buf, part).wait_send()

    def stat_copy(layer, d):
        return pltpu.make_async_remote_copy(
            src_ref=stat.at[layer, me], dst_ref=stat.at[layer, me],
            send_sem=st_send.at[layer, d], recv_sem=st_recv.at[layer, me],
            device_id=device(lax.rem(me + d, n_dev)), device_id_type=MESH)

    def stat_start(layer, s1, s2):
        stat[layer, me, 0:1, :] = jnp.sum(s1, axis=0, keepdims=True)
        stat[layer, me, 1:2, :] = jnp.sum(s2, axis=0, keepdims=True)
        for d in range(1, n_dev):
            stat_copy(layer, d).start()

    def stat_finish(layer):
        for d in range(1, n_dev):
            src = lax.rem(me + d, n_dev)
            pltpu.make_async_remote_copy(
                src_ref=stat.at[layer, src], dst_ref=stat.at[layer, src],
                send_sem=st_send.at[layer, d], recv_sem=st_recv.at[layer, src],
                device_id=device(src), device_id_type=MESH).wait_recv()
            stat_copy(layer, d).wait_send()
        lane = lax.broadcasted_iota(jnp.int32, (8, ch), 1)
        sums = jnp.sum(stat[layer], axis=0)
        s1 = group_sum(jnp.broadcast_to(sums[0:1], (8, ch)), lane)
        s2 = group_sum(jnp.broadcast_to(sums[1:2], (8, ch)), lane)
        mean = s1 / total
        inv = lax.rsqrt(s2 / total - mean * mean + EPS)
        scale = gamma_ref[pl.ds(layer, 1)] * inv
        shift = beta_ref[pl.ds(layer, 1)] - mean * scale
        return (0.5 * scale)[0:1], (0.5 * shift)[0:1]

    last = n_q - 1

    def stats_of(v, s1, s2):
        v8 = v.reshape(v.shape[0] // 8, 8, ch)
        return s1 + jnp.sum(v8, axis=0), s2 + jnp.sum(v8 * v8, axis=0)

    zero = jnp.zeros((8, ch), F32)

    def x_stats(k, carry):
        in_copy(k).wait()
        s1, s2 = carry
        for f in range(CHUNK):
            for r in range(rows):
                s1, s2 = stats_of(raw_a[k * CHUNK + 2 + f, r + 1].astype(F32), s1, s2)
        return s1, s2

    sums = lax.fori_loop(0, n_q, x_stats, (zero, zero))
    pl.semaphore_wait(barrier, n_dev - 1)
    stat_start(0, *sums)
    rows_start(range(n_q, -1, -1), 0)
    cp_start(0)

    sub = lax.broadcasted_iota(jnp.int32, (8, ch), 0)

    def norm_row(raw, frame, r, act, slot, scale, shift):
        t = raw[frame, r].astype(F32) * scale + shift
        v = t + t * jnp.tanh(t)
        if r == 0:
            v = jnp.where(has_up, v, 0.0)
        if r == rows + 1:
            v = jnp.where(has_down, v, 0.0)
        left, right = pltpu.roll(v, 1, 0), pltpu.roll(v, width - 1, 0)
        left = jnp.concatenate([jnp.where(sub == 0, 0.0, left[:8]), left[8:]], axis=0)
        right = jnp.concatenate([right[:-8], jnp.where(sub == 7, 0.0, right[-8:])], axis=0)
        act[slot, r, :, 0:ch] = left.astype(BF16)
        act[slot, r, :, ch:2 * ch] = v.astype(BF16)
        act[slot, r, :, 2 * ch:3 * ch] = right.astype(BF16)

    first_frame = jnp.where(has_prev, 0, 2)

    def step(q, block, sub_idx, par, scale, shift, carry):
        src = raws[sub_idx]
        act, nxt = (act_a, act_b) if par == 0 else (act_b, act_a)
        wa, wb = wts[sub_idx]
        base = jnp.maximum(q * CHUNK - CHUNK, 0)
        sums = [carry]

        def norm_item(f, r):
            frame = base + f if f >= 2 else jnp.maximum(base + f, first_frame)
            norm_row(src, frame, r, nxt, f, scale, shift)

        def tail_item(p, i):
            sums[0] = epilogue(q + 1, block, sub_idx, 1 - par, p, i, sums[0])

        norms = [functools.partial(norm_item, f, r) for f in range(CHUNK) for r in range(rows + 2)]
        tails = [functools.partial(tail_item, p, i) for i in range(rows) for p in range(2)]
        items = []
        for n in range(len(tails)):
            items += norms[3 * n:3 * n + 3] + [tails[n]]
        parts = [functools.partial(row_part, act, wb, n) for n in range(2)] + [functools.partial(time_part, act, wa, n) for n in range(3)]
        weight = [2, 2, 3, 3, 3]
        acc, done = {}, 0
        for n, part in enumerate(parts):
            for key, value in part():
                acc[key] = acc[key] + value if key in acc else value
            if n == 1:
                for p in range(2):
                    for o in range(2):
                        acc_r[par, p, o] = acc[p, o]
            upto = sum(weight[:n + 1]) * len(items) // sum(weight)
            for item in items[done:upto]:
                item()
            done = upto
        for p in range(2):
            acc_t[par, p] = acc[p]
        nxt[CHUNK:CHUNK + 2] = act[0:2]
        return sums[0]

    def row_part(act, wb, n):
        for o in range(2):
            taps = [divmod(t, 3) for t in range(6 * n, 6 * n + 6)]
            weights = jnp.concatenate([wb[o, i, j] for i, j in taps], axis=0)
            for p in range(2):
                lhs = jnp.concatenate([
                    jnp.concatenate([act[2 * p + 3 * o, r + i, :, j * ch:(j + 1) * ch] for i, j in taps], axis=1)
                    for r in range(0, rows, 2)], axis=0)
                yield (p, o), jnp.dot(lhs, weights, preferred_element_type=F32)

    def time_part(act, wa, n):
        taps = [(t // 9, t // 3 % 3, t % 3) for t in range(6 * n, 6 * n + 6)]
        weights = jnp.concatenate([wa[k, i, j] for k, i, j in taps], axis=0)
        for p in range(2):
            lhs = jnp.concatenate([act[2 * p + 1 + k, i:i + rows, :, j * ch:(j + 1) * ch].reshape(rows * width, ch)
                                   for k, i, j in taps], axis=1)
            yield p, jnp.dot(lhs, weights, preferred_element_type=F32)

    def epilogue(q, block, sub_idx, par, p, i, sums):
        dst = raws[1 - sub_idx]
        acc = acc_t[par, p, i * width:(i + 1) * width]
        bias = bias_ref[pl.ds(2 * block + sub_idx, 1)]
        for o in range(2):
            two = acc_r[par, p, o, i // 2 * width:(i // 2 + 1) * width, i % 2 * ch:(i % 2 + 1) * ch]
            y = (acc[:, o * ch:(o + 1) * ch] + two + bias).astype(BF16)
            frame = q * CHUNK + 2 + 2 * p + o
            if sub_idx == 1:
                y = (dst[frame, i + 1].astype(F32) + y.astype(F32)).astype(BF16)
            dst[frame, i + 1] = y
            sums = stats_of(y.astype(F32), *sums)
        return sums

    def conv_layer(block, sub_idx, scale, shift):
        src = raws[sub_idx]
        for cp in w_copies(sub_idx, sub_idx):
            cp.wait()
        rows_wait((n_q, last), sub_idx)
        for f in range(CHUNK + 2):
            for r in range(rows + 2):
                norm_row(src, frames - CHUNK + f, r, act_a, f, scale, shift)

        def pair(i, carry):
            q = last - 2 * i

            @pl.when(i < n_q // 2 - 1)
            def _():
                rows_wait((q - 1, q - 2), sub_idx)

            @pl.when(i == n_q // 2 - 1)
            def _():
                rows_wait((0,), sub_idx)
                cp_wait(sub_idx)

            send(i, q, block, sub_idx)
            s1, s2 = step(q, block, sub_idx, 0, scale, shift, carry)
            carry = jnp.where(i == 0, 0.0, s1), jnp.where(i == 0, 0.0, s2)
            return step(q - 1, block, sub_idx, 1, scale, shift, carry)

        sums = lax.fori_loop(0, n_q // 2, pair, (zero, zero))
        for i in range(rows):
            for p in range(2):
                sums = epilogue(0, block, sub_idx, 1, p, i, sums)
        return sums

    def send(i, q, block, sub_idx):
        buf = 1 - sub_idx
        more = True if sub_idx == 0 else block == 0

        @pl.when((i == 1) & more)
        def _():
            rows_start((n_q,), buf)
            cp_start(buf)

        @pl.when((i > 1) & more)
        def _():
            rows_start((q + 4, q + 3), buf)

        if sub_idx == 1:
            @pl.when((i == 1) & (block == 1))
            def _():
                out_copy(last).start()

            @pl.when((i > 1) & (block == 1))
            def _():
                out_copy(q + 3).start()
                out_copy(q + 2).start()

    def send_rest(block, sub_idx):
        if sub_idx == 0:
            rows_start((3, 2, 1, 0), 1)
        else:
            @pl.when(block == 0)
            def _():
                rows_start((3, 2, 1, 0), 0)

            @pl.when(block == 1)
            def _():
                for q in (2, 1, 0):
                    out_copy(q).start()

    def out_copy(q):
        return pltpu.make_async_copy(raw_a.at[pl.ds(q * CHUNK + 2, CHUNK), 1:rows + 1],
                                     out_ref.at[pl.ds(q * CHUNK, CHUNK)], out_sem.at[q])

    def block_body(block, _):
        scale, shift = stat_finish(2 * block)
        sums = conv_layer(block, 0, scale, shift)
        stat_start(2 * block + 1, *sums)
        send_rest(block, 0)

        @pl.when(block == 0)
        def _():
            for cp in w_copies(2, 0):
                cp.start()

        scale, shift = stat_finish(2 * block + 1)
        sums = conv_layer(block, 1, scale, shift)

        @pl.when(block == 0)
        def _():
            stat_start(2, *sums)
            for cp in w_copies(3, 1):
                cp.start()

        send_rest(block, 1)
        return 0

    lax.fori_loop(0, 2, block_body, 0)
    for q in range(n_q):
        out_copy(q).wait()


def solution(mesh):
    n_h, n_c = mesh.shape["hp"], mesh.shape["cp"]

    def local_decode(lat, conv_w, conv_b, gamma, beta):
        frames, rows, width, ch = lat.shape
        total = float(frames * n_c * rows * n_h * width * (ch // GROUPS))
        n_q = frames // CHUNK
        cfg = (n_h, n_c, frames, rows, width, ch, total)
        vmem = pl.BlockSpec(memory_space=pltpu.VMEM)
        hbm = pl.BlockSpec(memory_space=pltpu.HBM)
        dma = pltpu.SemaphoreType.DMA
        return pl.pallas_call(
            functools.partial(kernel, cfg),
            out_shape=jax.ShapeDtypeStruct(lat.shape, lat.dtype),
            in_specs=[hbm, hbm, vmem, vmem, vmem],
            out_specs=pl.BlockSpec(memory_space=pl.ANY),
            scratch_shapes=[
                pltpu.VMEM((frames + 2 + CHUNK, rows + 2, width, ch), BF16),
                pltpu.VMEM((frames + 2 + CHUNK, rows + 2, width, ch), BF16),
                pltpu.VMEM((CHUNK + 2, rows + 2, width, 3 * ch), BF16),
                pltpu.VMEM((CHUNK + 2, rows + 2, width, 3 * ch), BF16),
                pltpu.VMEM((2, 3, 3, ch, 2 * ch), BF16),
                pltpu.VMEM((2, 3, 3, ch, 2 * ch), BF16),
                pltpu.VMEM((2, 4, 3, ch, 2 * ch), BF16),
                pltpu.VMEM((2, 4, 3, ch, 2 * ch), BF16),
                pltpu.VMEM((2, 2, rows * width, 2 * ch), F32),
                pltpu.VMEM((2, 2, 2, rows // 2 * width, 2 * ch), F32),
                pltpu.VMEM((4, n_h * n_c, 2, ch), F32),
                dma((n_q,)), dma((n_q,)), dma((2, 6)),
                dma((2, 2, n_q + 1)), dma((2, 2, n_q + 1)), dma((2, 3)), dma((2, 3)),
                dma((4, n_h * n_c)), dma((4, n_h * n_c)),
            ],
            compiler_params=pltpu.CompilerParams(collective_id=0, has_side_effects=True, vmem_limit_bytes=46 * 1024 * 1024),
        )(lat, conv_w, conv_b, gamma, beta)

    spec = P(("dp", "cp"), "hp", None, None)
    return jax.shard_map(local_decode, mesh=mesh, in_specs=(spec, P(), P(), P(), P()), out_specs=spec, check_vma=False)
```

```python
import functools

import jax
import jax.numpy as jnp
from jax import lax
from jax.experimental import pallas as pl
from jax.experimental.pallas import tpu as pltpu
from jax.sharding import PartitionSpec as P

GROUPS = 32
EPS = 1e-6
CHUNK = 4
MESH = pl.DeviceIdType.MESH
F32 = jnp.float32
BF16 = jnp.bfloat16


def group_sum(v, lane):
    n = v.shape[-1]
    v = v + jnp.where(lane % 2 == 0, pltpu.roll(v, n - 1, 1), pltpu.roll(v, 1, 1))
    return v + jnp.where(lane % 4 < 2, pltpu.roll(v, n - 2, 1), pltpu.roll(v, 2, 1))


def kernel(cfg, lat_ref, w_ref, bias_ref, gamma_ref, beta_ref, out_ref, raw_a, raw_b, act_a, act_b, wa_a, wa_b, wb_a, wb_b, acc_t, acc_r, stat,
           in_sem, w_sem, row_send, row_recv, cp_send, cp_recv, st_send, st_recv):
    n_h, n_c, frames, rows, width, ch, total = cfg
    n_q = frames // CHUNK
    n_dev = n_h * n_c
    h = lax.axis_index("hp")
    c = lax.axis_index("cp")
    me = h * n_c + c
    has_up, has_down = h > 0, h < n_h - 1
    has_prev, has_next = c > 0, c < n_c - 1

    def device(idx):
        return {"hp": idx // n_c, "cp": lax.rem(idx, n_c)}

    barrier = pltpu.get_barrier_semaphore()
    for d in range(1, n_dev):
        pl.semaphore_signal(barrier, inc=1, device_id=device(lax.rem(me + d, n_dev)), device_id_type=MESH)

    def in_copy(k):
        return pltpu.make_async_copy(lat_ref.at[pl.ds(k * CHUNK, CHUNK)],
                                     raw_a.at[pl.ds(k * CHUNK + 2, CHUNK), 1:rows + 1], in_sem.at[k])

    for k in range(n_q):
        in_copy(k).start()

    wts = ((wa_a, wb_a), (wa_b, wb_b))

    def w_copies(layer, which):
        wa, wb = wts[which]
        pairs = [(w_ref.at[layer, 1:3], wa.at[0]), (w_ref.at[layer, 0:2], wa.at[1])]
        for o in range(2):
            for n in range(2):
                pairs.append((w_ref.at[layer, 2 * o], wb.at[n, o, n:n + 3]))
        return [pltpu.make_async_copy(src, dst, w_sem.at[which, n]) for n, (src, dst) in enumerate(pairs)]

    for which in range(2):
        wb = wts[which][1]
        for o in range(2):
            for j in range(3):
                for n in range(2):
                    wb[n, o, 3 - 3 * n, j] = jnp.zeros((ch, ch), BF16)
    raws = (raw_a, raw_b)

    def row_copy(k, buf, up):
        fr = {0: pl.ds(2, CHUNK - 2), n_q: pl.ds(frames, 2)}.get(k, pl.ds(k * CHUNK, CHUNK)) if isinstance(k, int) else pl.ds(k * CHUNK, CHUNK)
        d = 0 if up else 1
        return pltpu.make_async_remote_copy(
            src_ref=raws[buf].at[fr, 1 if up else rows], dst_ref=raws[buf].at[fr, rows + 1 if up else 0],
            send_sem=row_send.at[buf, d, k], recv_sem=row_recv.at[buf, d, k],
            device_id={"hp": h - 1 if up else h + 1}, device_id_type=MESH)

    def rows_start(chunks, buf, gate=True):
        for up, cond in ((True, has_up), (False, has_down)):
            @pl.when(cond & gate)
            def _():
                for k in chunks:
                    row_copy(k, buf, up).start()

    def rows_wait(chunks, buf):
        for up, cond in ((True, has_down), (False, has_up)):
            @pl.when(cond)
            def _():
                for k in chunks:
                    row_copy(k, buf, up).wait_recv()
                    row_copy(k, buf, not up).wait_send()

    def cp_copy(buf, part, src=None):
        lo, hi, dst_lo, dst_hi, dh = ((0, rows, 1, rows + 1, 0), (0, 1, rows + 1, rows + 2, -1),
                                      (rows - 1, rows, 0, 1, 1))[part]
        source = raws[buf].at[frames:frames + 2, lo + 1:hi + 1] if src is None else src.at[frames - 2:frames, lo:hi]
        return pltpu.make_async_remote_copy(
            src_ref=source, dst_ref=raws[buf].at[0:2, dst_lo:dst_hi],
            send_sem=cp_send.at[buf, part], recv_sem=cp_recv.at[buf, part],
            device_id={"hp": h + dh, "cp": c + 1}, device_id_type=MESH)

    def cp_start(buf, src=None):
        for part, cond in enumerate((has_next, has_next & has_up, has_next & has_down)):
            @pl.when(cond)
            def _():
                cp_copy(buf, part, src).start()

    def cp_wait(buf):
        for part, cond in enumerate((has_prev, has_prev & has_down, has_prev & has_up)):
            @pl.when(cond)
            def _():
                cp_copy(buf, part).wait_recv()
        for part, cond in enumerate((has_next, has_next & has_up, has_next & has_down)):
            @pl.when(cond)
            def _():
                cp_copy(buf, part).wait_send()

    def stat_copy(layer, d):
        return pltpu.make_async_remote_copy(
            src_ref=stat.at[layer, me], dst_ref=stat.at[layer, me],
            send_sem=st_send.at[layer, d], recv_sem=st_recv.at[layer, me],
            device_id=device(lax.rem(me + d, n_dev)), device_id_type=MESH)

    def stat_start(layer, s1, s2):
        stat[layer, me, 0:1, :] = jnp.sum(s1, axis=0, keepdims=True)
        stat[layer, me, 1:2, :] = jnp.sum(s2, axis=0, keepdims=True)
        for d in range(1, n_dev):
            stat_copy(layer, d).start()

    def stat_finish(layer):
        for d in range(1, n_dev):
            src = lax.rem(me + d, n_dev)
            pltpu.make_async_remote_copy(
                src_ref=stat.at[layer, src], dst_ref=stat.at[layer, src],
                send_sem=st_send.at[layer, d], recv_sem=st_recv.at[layer, src],
                device_id=device(src), device_id_type=MESH).wait_recv()
        lane = lax.broadcasted_iota(jnp.int32, (8, ch), 1)
        sums = jnp.sum(stat[layer], axis=0)
        s1 = group_sum(jnp.broadcast_to(sums[0:1], (8, ch)), lane)
        s2 = group_sum(jnp.broadcast_to(sums[1:2], (8, ch)), lane)
        mean = s1 / total
        inv = lax.rsqrt(s2 / total - mean * mean + EPS)
        scale = gamma_ref[pl.ds(layer, 1)] * inv
        shift = beta_ref[pl.ds(layer, 1)] - mean * scale
        return (0.5 * scale)[0:1], (0.5 * shift)[0:1]

    last = n_q - 1

    def stats_of(v, s1, s2):
        v8 = v.reshape(v.shape[0] // 8, 8, ch)
        return s1 + jnp.sum(v8, axis=0), s2 + jnp.sum(v8 * v8, axis=0)

    zero = jnp.zeros((8, ch), F32)

    def x_stats(k, carry):
        in_copy(k).wait()
        s1, s2 = carry
        for f in range(CHUNK):
            for r in range(rows):
                s1, s2 = stats_of(raw_a[k * CHUNK + 2 + f, r + 1].astype(F32), s1, s2)
        return s1, s2

    sums = lax.fori_loop(0, n_q, x_stats, (zero, zero))
    for which in range(2):
        for cp in w_copies(which, which):
            cp.start()
    pl.semaphore_wait(barrier, n_dev - 1)
    stat_start(0, *sums)
    rows_start(range(n_q, -1, -1), 0)
    cp_start(0)

    sub = lax.broadcasted_iota(jnp.int32, (8, ch), 0)

    def norm_row(raw, frame, r, act, slot, scale, shift):
        t = raw[frame, r].astype(F32) * scale + shift
        v = t + t * jnp.tanh(t)
        if r == 0:
            v = jnp.where(has_up, v, 0.0)
        if r == rows + 1:
            v = jnp.where(has_down, v, 0.0)
        left, right = pltpu.roll(v, 1, 0), pltpu.roll(v, width - 1, 0)
        left = jnp.concatenate([jnp.where(sub == 0, 0.0, left[:8]), left[8:]], axis=0)
        right = jnp.concatenate([right[:-8], jnp.where(sub == 7, 0.0, right[-8:])], axis=0)
        act[slot, r, 0] = left.astype(BF16)
        act[slot, r, 1] = v.astype(BF16)
        act[slot, r, 2] = right.astype(BF16)

    first_frame = jnp.where(has_prev, 0, 2)

    def step(q, block, sub_idx, par, scale, shift, carry, first=False):
        src = raws[sub_idx]
        act, nxt = (act_a, act_b) if par == 0 else (act_b, act_a)
        wa, wb = wts[sub_idx]
        base = jnp.maximum(q * CHUNK - CHUNK, 0)
        sums = [carry]

        def norm_item(f, r):
            frame = base + f if f >= 2 else jnp.maximum(base + f, first_frame)
            norm_row(src, frame, r, nxt, f, scale, shift)

        def tail_item(p, i):
            sums[0] = epilogue(q + 1, block, sub_idx, 1 - par, p, i, sums[0])

        norms = [functools.partial(norm_item, f, r) for f in range(CHUNK) for r in range(rows + 2)]
        tails = [functools.partial(tail_item, p, i) for i in range(rows) for p in range(2)]
        parts = ([functools.partial(row_part, act, wb, o, n) for o in range(2) for n in range(2)]
                 + [functools.partial(time_part, act, wa, n) for n in range(3)])
        if first:
            def own(f):
                return [functools.partial(norm_row, src, frames - CHUNK + f, r, act, f, scale, shift) for r in range(rows + 2)]

            for item in own(0) + own(2):
                item()
            beside = [own(3), own(5), own(1), own(4), norms[:8], norms[8:16], norms[16:]]
        else:
            items = []
            for n in range(len(tails)):
                items += norms[3 * n:3 * n + 3] + [tails[n]]
            edges = [len(items) * n // 10 for n in (0, 1, 2, 3, 4, 6, 8, 10)]
            beside = [items[lo:hi] for lo, hi in zip(edges, edges[1:])]
        acc = {}
        for n, part in enumerate(parts):
            for key, value in part():
                acc[key] = acc[key] + value if key in acc else value
            if n in (1, 3):
                for p in range(2):
                    acc_r[par, p, n // 2] = acc[p, n // 2]
            for item in beside[n]:
                item()
        for p in range(2):
            acc_t[par, p] = acc[p]
        nxt[CHUNK:CHUNK + 2] = act[0:2]
        return sums[0]

    def row_part(act, wb, o, n):
        taps = [divmod(t, 3) for t in range(6 * n, 6 * n + 6)]
        weights = jnp.concatenate([jnp.concatenate([wb[n2, o, i, j] for i, j in taps], axis=0) for n2 in range(2)], axis=1)
        for p in range(2):
            lhs = jnp.concatenate([
                jnp.concatenate([act[2 * p + 3 * o, r + i, j] for i, j in taps], axis=1)
                for r in range(0, rows, 2)], axis=0)
            yield (p, o), jnp.dot(lhs, weights, preferred_element_type=F32)

    def time_part(act, wa, n):
        taps = [(t // 9, t // 3 % 3, t % 3) for t in range(6 * n, 6 * n + 6)]
        weights = jnp.concatenate([jnp.concatenate([wa[n2, k, i, j] for k, i, j in taps], axis=0) for n2 in range(2)], axis=1)
        for p in range(2):
            lhs = jnp.concatenate([act[2 * p + 1 + k, i:i + rows, j].reshape(rows * width, ch)
                                   for k, i, j in taps], axis=1)
            yield p, jnp.dot(lhs, weights, preferred_element_type=F32)

    def epilogue(q, block, sub_idx, par, p, i, sums):
        dst = raws[1 - sub_idx]
        acc = acc_t[par, p, i * width:(i + 1) * width]
        bias = bias_ref[pl.ds(2 * block + sub_idx, 1)]
        for o in range(2):
            two = acc_r[par, p, o, i // 2 * width:(i // 2 + 1) * width, i % 2 * ch:(i % 2 + 1) * ch]
            y = (acc[:, o * ch:(o + 1) * ch] + two + bias).astype(BF16)
            frame = q * CHUNK + 2 + 2 * p + o
            if sub_idx == 1:
                y = (dst[frame, i + 1].astype(F32) + y.astype(F32)).astype(BF16)
            dst[frame, i + 1] = y
            if sub_idx == 1:
                out_ref[frame - 2, i] = y
            sums = stats_of(y.astype(F32), *sums)
        return sums

    def conv_layer(block, sub_idx, scale, shift):
        src = raws[sub_idx]
        for cp in w_copies(sub_idx, sub_idx):
            cp.wait()
        rows_wait((n_q, last, last - 1, last - 2), sub_idx)
        carry = step(last, block, sub_idx, 0, scale, shift, (zero, zero), first=True)
        carry = step(last - 1, block, sub_idx, 1, scale, shift, carry)

        def pair(i, carry):
            q = last - 2 * i

            @pl.when(i < n_q // 2 - 1)
            def _():
                rows_wait((q - 1, q - 2), sub_idx)

            @pl.when(i == n_q // 2 - 1)
            def _():
                rows_wait((0,), sub_idx)
                cp_wait(sub_idx)

            send(i, q, block, sub_idx)
            carry = step(q, block, sub_idx, 0, scale, shift, carry)
            return step(q - 1, block, sub_idx, 1, scale, shift, carry)

        sums = lax.fori_loop(1, n_q // 2, pair, carry)
        for i in range(rows):
            for p in range(2):
                sums = epilogue(0, block, sub_idx, 1, p, i, sums)
        return sums

    def send(i, q, block, sub_idx):
        buf = 1 - sub_idx
        more = True if sub_idx == 0 else block == 0

        @pl.when((i == 1) & more)
        def _():
            rows_start((n_q,), buf)
            cp_start(buf)

        rows_start((7, 6), buf, (i == 2) & more)
        rows_start((5,), buf, (i == 3) & more)

    def send_rest(block, sub_idx):
        if sub_idx == 0:
            rows_start((4, 3, 2, 1, 0), 1)
        else:
            @pl.when(block == 0)
            def _():
                rows_start((4, 3, 2, 1, 0), 0)

    def block_body(block, _):
        scale, shift = stat_finish(2 * block)
        sums = conv_layer(block, 0, scale, shift)
        stat_start(2 * block + 1, *sums)
        send_rest(block, 0)

        @pl.when(block == 0)
        def _():
            for cp in w_copies(2, 0):
                cp.start()

        scale, shift = stat_finish(2 * block + 1)
        sums = conv_layer(block, 1, scale, shift)

        @pl.when(block == 0)
        def _():
            stat_start(2, *sums)
            for cp in w_copies(3, 1):
                cp.start()

        send_rest(block, 1)
        return 0

    lax.fori_loop(0, 2, block_body, 0)
    for layer in range(4):
        for d in range(1, n_dev):
            stat_copy(layer, d).wait_send()


def solution(mesh):
    n_h, n_c = mesh.shape["hp"], mesh.shape["cp"]

    def local_decode(lat, conv_w, conv_b, gamma, beta):
        frames, rows, width, ch = lat.shape
        total = float(frames * n_c * rows * n_h * width * (ch // GROUPS))
        n_q = frames // CHUNK
        cfg = (n_h, n_c, frames, rows, width, ch, total)
        vmem = pl.BlockSpec(memory_space=pltpu.VMEM)
        hbm = pl.BlockSpec(memory_space=pltpu.HBM)
        dma = pltpu.SemaphoreType.DMA
        return pl.pallas_call(
            functools.partial(kernel, cfg),
            out_shape=jax.ShapeDtypeStruct(lat.shape, lat.dtype),
            in_specs=[hbm, hbm, vmem, vmem, vmem],
            out_specs=vmem,
            scratch_shapes=[
                pltpu.VMEM((frames + 2 + CHUNK, rows + 2, width, ch), BF16),
                pltpu.VMEM((frames + 2 + CHUNK, rows + 2, width, ch), BF16),
                pltpu.VMEM((CHUNK + 2, rows + 2, 3, width, ch), BF16),
                pltpu.VMEM((CHUNK + 2, rows + 2, 3, width, ch), BF16),
                pltpu.VMEM((2, 2, 3, 3, ch, ch), BF16),
                pltpu.VMEM((2, 2, 3, 3, ch, ch), BF16),
                pltpu.VMEM((2, 2, 4, 3, ch, ch), BF16),
                pltpu.VMEM((2, 2, 4, 3, ch, ch), BF16),
                pltpu.VMEM((2, 2, rows * width, 2 * ch), F32),
                pltpu.VMEM((2, 2, 2, rows // 2 * width, 2 * ch), F32),
                pltpu.VMEM((4, n_h * n_c, 2, ch), F32),
                dma((n_q,)), dma((2, 6)),
                dma((2, 2, n_q + 1)), dma((2, 2, n_q + 1)), dma((2, 3)), dma((2, 3)),
                dma((4, n_h * n_c)), dma((4, n_h * n_c)),
            ],
            compiler_params=pltpu.CompilerParams(collective_id=0, has_side_effects=True, vmem_limit_bytes=50 * 1024 * 1024),
        )(lat, conv_w, conv_b, gamma, beta)

    spec = P(("dp", "cp"), "hp", None, None)
    return jax.shard_map(local_decode, mesh=mesh, in_specs=(spec, P(), P(), P(), P()), out_specs=spec, check_vma=False)
```

```python
import functools

import jax
import jax.numpy as jnp
from jax import lax
from jax.experimental import pallas as pl
from jax.experimental.pallas import tpu as pltpu
from jax.sharding import PartitionSpec as P

GROUPS = 32
EPS = 1e-6
CHUNK = 4
MESH = pl.DeviceIdType.MESH
F32 = jnp.float32
BF16 = jnp.bfloat16


def group_sum(v, lane):
    n = v.shape[-1]
    v = v + jnp.where(lane % 2 == 0, pltpu.roll(v, n - 1, 1), pltpu.roll(v, 1, 1))
    return v + jnp.where(lane % 4 < 2, pltpu.roll(v, n - 2, 1), pltpu.roll(v, 2, 1))


def kernel(cfg, lat_ref, w_ref, bias_ref, gamma_ref, beta_ref, out_ref, raw_a, raw_b, act_a, act_b, wa_a, wa_b, wb_a, wb_b, acc_t, acc_r, stat,
           in_sem, w_sem, row_send, row_recv, cp_send, cp_recv, st_send, st_recv):
    n_h, n_c, frames, rows, width, ch, total = cfg
    n_q = frames // CHUNK
    n_dev = n_h * n_c
    h = lax.axis_index("hp")
    c = lax.axis_index("cp")
    me = h * n_c + c
    has_up, has_down = h > 0, h < n_h - 1
    has_prev, has_next = c > 0, c < n_c - 1

    def device(idx):
        return {"hp": idx // n_c, "cp": lax.rem(idx, n_c)}

    barrier = pltpu.get_barrier_semaphore()
    for d in range(1, n_dev):
        pl.semaphore_signal(barrier, inc=1, device_id=device(lax.rem(me + d, n_dev)), device_id_type=MESH)

    def in_copy(k):
        return pltpu.make_async_copy(lat_ref.at[pl.ds(k * CHUNK, CHUNK)],
                                     raw_a.at[pl.ds(k * CHUNK + 2, CHUNK), 1:rows + 1], in_sem.at[k])

    for k in range(n_q):
        in_copy(k).start()

    wts = ((wa_a, wb_a), (wa_b, wb_b))

    def w_copies(layer, which):
        wa, wb = wts[which]
        pairs = [(w_ref.at[layer, 1:3], wa.at[0]), (w_ref.at[layer, 0:2], wa.at[1])]
        for o in range(2):
            for n in range(2):
                pairs.append((w_ref.at[layer, 2 * o], wb.at[n, o, n:n + 3]))
        return [pltpu.make_async_copy(src, dst, w_sem.at[which, n]) for n, (src, dst) in enumerate(pairs)]

    for which in range(2):
        wb = wts[which][1]
        for o in range(2):
            for j in range(3):
                for n in range(2):
                    wb[n, o, 3 - 3 * n, j] = jnp.zeros((ch, ch), BF16)
    raws = (raw_a, raw_b)

    def row_copy(k, buf, up):
        fr = {0: pl.ds(2, CHUNK - 2), n_q: pl.ds(frames, 2)}.get(k, pl.ds(k * CHUNK, CHUNK)) if isinstance(k, int) else pl.ds(k * CHUNK, CHUNK)
        d = 0 if up else 1
        return pltpu.make_async_remote_copy(
            src_ref=raws[buf].at[fr, 1 if up else rows], dst_ref=raws[buf].at[fr, rows + 1 if up else 0],
            send_sem=row_send.at[buf, d, k], recv_sem=row_recv.at[buf, d, k],
            device_id={"hp": h - 1 if up else h + 1}, device_id_type=MESH)

    def rows_start(chunks, buf, gate=True):
        for up, cond in ((True, has_up), (False, has_down)):
            @pl.when(cond & gate)
            def _():
                for k in chunks:
                    row_copy(k, buf, up).start()

    def rows_wait(chunks, buf):
        for up, cond in ((True, has_down), (False, has_up)):
            @pl.when(cond)
            def _():
                for k in chunks:
                    row_copy(k, buf, up).wait_recv()
                    row_copy(k, buf, not up).wait_send()

    def cp_copy(buf, part, src=None):
        lo, hi, dst_lo, dst_hi, dh = ((0, rows, 1, rows + 1, 0), (0, 1, rows + 1, rows + 2, -1),
                                      (rows - 1, rows, 0, 1, 1))[part]
        source = raws[buf].at[frames:frames + 2, lo + 1:hi + 1] if src is None else src.at[frames - 2:frames, lo:hi]
        return pltpu.make_async_remote_copy(
            src_ref=source, dst_ref=raws[buf].at[0:2, dst_lo:dst_hi],
            send_sem=cp_send.at[buf, part], recv_sem=cp_recv.at[buf, part],
            device_id={"hp": h + dh, "cp": c + 1}, device_id_type=MESH)

    def cp_start(buf, src=None):
        for part, cond in enumerate((has_next, has_next & has_up, has_next & has_down)):
            @pl.when(cond)
            def _():
                cp_copy(buf, part, src).start()

    def cp_wait(buf):
        for part, cond in enumerate((has_prev, has_prev & has_down, has_prev & has_up)):
            @pl.when(cond)
            def _():
                cp_copy(buf, part).wait_recv()
        for part, cond in enumerate((has_next, has_next & has_up, has_next & has_down)):
            @pl.when(cond)
            def _():
                cp_copy(buf, part).wait_send()

    def stat_copy(layer, d):
        return pltpu.make_async_remote_copy(
            src_ref=stat.at[layer, me], dst_ref=stat.at[layer, me],
            send_sem=st_send.at[layer, d], recv_sem=st_recv.at[layer, me],
            device_id=device(lax.rem(me + d, n_dev)), device_id_type=MESH)

    def stat_start(layer, s1, s2):
        stat[layer, me, 0:1, :] = jnp.sum(s1, axis=0, keepdims=True)
        stat[layer, me, 1:2, :] = jnp.sum(s2, axis=0, keepdims=True)
        for d in range(1, n_dev):
            stat_copy(layer, d).start()

    def stat_finish(layer):
        for d in range(1, n_dev):
            src = lax.rem(me + d, n_dev)
            pltpu.make_async_remote_copy(
                src_ref=stat.at[layer, src], dst_ref=stat.at[layer, src],
                send_sem=st_send.at[layer, d], recv_sem=st_recv.at[layer, src],
                device_id=device(src), device_id_type=MESH).wait_recv()
        lane = lax.broadcasted_iota(jnp.int32, (8, ch), 1)
        sums = jnp.sum(stat[layer], axis=0)
        s1 = group_sum(jnp.broadcast_to(sums[0:1], (8, ch)), lane)
        s2 = group_sum(jnp.broadcast_to(sums[1:2], (8, ch)), lane)
        mean = s1 / total
        inv = lax.rsqrt(s2 / total - mean * mean + EPS)
        scale = gamma_ref[pl.ds(layer, 1)] * inv
        shift = beta_ref[pl.ds(layer, 1)] - mean * scale
        return (0.5 * scale)[0:1], (0.5 * shift)[0:1]

    last = n_q - 1

    def stats_of(v, s1, s2):
        v8 = v.reshape(v.shape[0] // 8, 8, ch)
        return s1 + jnp.sum(v8, axis=0), s2 + jnp.sum(v8 * v8, axis=0)

    zero = jnp.zeros((8, ch), F32)

    def x_stats(k, carry):
        in_copy(k).wait()
        s1, s2 = carry
        for f in range(CHUNK):
            for r in range(rows):
                s1, s2 = stats_of(raw_a[k * CHUNK + 2 + f, r + 1].astype(F32), s1, s2)
        return s1, s2

    sums = lax.fori_loop(0, n_q, x_stats, (zero, zero))
    for which in range(2):
        for cp in w_copies(which, which):
            cp.start()
    pl.semaphore_wait(barrier, n_dev - 1)
    stat_start(0, *sums)
    rows_start(range(n_q, -1, -1), 0)
    cp_start(0)

    sub = lax.broadcasted_iota(jnp.int32, (8, ch), 0)

    def norm_row(raw, frame, r, act, slot, scale, shift):
        t = raw[frame, r].astype(F32) * scale + shift
        v = t + t * jnp.tanh(t)
        if r == 0:
            v = jnp.where(has_up, v, 0.0)
        if r == rows + 1:
            v = jnp.where(has_down, v, 0.0)
        left, right = pltpu.roll(v, 1, 0), pltpu.roll(v, width - 1, 0)
        left = jnp.concatenate([jnp.where(sub == 0, 0.0, left[:8]), left[8:]], axis=0)
        right = jnp.concatenate([right[:-8], jnp.where(sub == 7, 0.0, right[-8:])], axis=0)
        act[slot, r, 0] = left.astype(BF16)
        act[slot, r, 1] = v.astype(BF16)
        act[slot, r, 2] = right.astype(BF16)

    first_frame = jnp.where(has_prev, 0, 2)

    def step(q, block, sub_idx, par, scale, shift, carry, first=False):
        src = raws[sub_idx]
        act, nxt = (act_a, act_b) if par == 0 else (act_b, act_a)
        wa, wb = wts[sub_idx]
        base = jnp.maximum(q * CHUNK - CHUNK, 0)
        sums = [carry]

        def norm_item(f, r):
            frame = base + f if f >= 2 else jnp.maximum(base + f, first_frame)
            norm_row(src, frame, r, nxt, f, scale, shift)

        def tail_item(p, i):
            sums[0] = epilogue(q + 1, block, sub_idx, 1 - par, p, i, sums[0])

        norms = [functools.partial(norm_item, f, r) for f in range(CHUNK) for r in range(rows + 2)]
        tails = [functools.partial(tail_item, p, i) for i in range(rows) for p in range(2)]
        parts = ([functools.partial(row_part, act, wb, o, n) for o in range(2) for n in range(2)]
                 + [functools.partial(time_part, act, wa, n) for n in range(3)])
        if first:
            def own(f):
                return [functools.partial(norm_row, src, frames - CHUNK + f, r, act, f, scale, shift) for r in range(rows + 2)]

            for item in own(0) + own(2):
                item()
            beside = [own(3), own(5), own(1), own(4), norms[:8], norms[8:16], norms[16:]]
        else:
            items = []
            for n in range(len(tails)):
                items += norms[3 * n:3 * n + 3] + [tails[n]]
            edges = [len(items) * n // 10 for n in (0, 1, 2, 3, 4, 6, 8, 10)]
            beside = [items[lo:hi] for lo, hi in zip(edges, edges[1:])]
        acc = {}
        for n, part in enumerate(parts):
            for key, value in part():
                acc[key] = acc[key] + value if key in acc else value
            if n in (1, 3):
                for p in range(2):
                    acc_r[par, p, n // 2] = acc[p, n // 2]
            for item in beside[n]:
                item()
        for p in range(2):
            acc_t[par, p] = acc[p]
        nxt[CHUNK:CHUNK + 2] = act[0:2]
        return sums[0]

    def row_part(act, wb, o, n):
        taps = [divmod(t, 3) for t in range(6 * n, 6 * n + 6)]
        weights = jnp.concatenate([jnp.concatenate([wb[n2, o, i, j] for i, j in taps], axis=0) for n2 in range(2)], axis=1)
        for p in range(2):
            lhs = jnp.concatenate([
                jnp.concatenate([act[2 * p + 3 * o, r + i, j] for i, j in taps], axis=1)
                for r in range(0, rows, 2)], axis=0)
            yield (p, o), jnp.dot(lhs, weights, preferred_element_type=F32)

    def time_part(act, wa, n):
        taps = [(t // 9, t // 3 % 3, t % 3) for t in range(6 * n, 6 * n + 6)]
        weights = jnp.concatenate([jnp.concatenate([wa[n2, k, i, j] for k, i, j in taps], axis=0) for n2 in range(2)], axis=1)
        for p in range(2):
            lhs = jnp.concatenate([act[2 * p + 1 + k, i:i + rows, j].reshape(rows * width, ch)
                                   for k, i, j in taps], axis=1)
            yield p, jnp.dot(lhs, weights, preferred_element_type=F32)

    def epilogue(q, block, sub_idx, par, p, i, sums):
        dst = raws[1 - sub_idx]
        acc = acc_t[par, p, i * width:(i + 1) * width]
        bias = bias_ref[pl.ds(2 * block + sub_idx, 1)]
        for o in range(2):
            two = acc_r[par, p, o, i // 2 * width:(i // 2 + 1) * width, i % 2 * ch:(i % 2 + 1) * ch]
            y = (acc[:, o * ch:(o + 1) * ch] + two + bias).astype(BF16)
            frame = q * CHUNK + 2 + 2 * p + o
            if sub_idx == 1:
                y = (dst[frame, i + 1].astype(F32) + y.astype(F32)).astype(BF16)
            dst[frame, i + 1] = y
            if sub_idx == 1:
                out_ref[frame - 2, i] = y
            sums = stats_of(y.astype(F32), *sums)
        return sums

    def conv_layer(block, sub_idx, scale, shift):
        src = raws[sub_idx]
        for cp in w_copies(sub_idx, sub_idx):
            cp.wait()
        rows_wait((n_q, last, last - 1, last - 2), sub_idx)
        carry = step(last, block, sub_idx, 0, scale, shift, (zero, zero), first=True)
        carry = step(last - 1, block, sub_idx, 1, scale, shift, carry)

        def pair(i, carry):
            q = last - 2 * i

            @pl.when(i < n_q // 2 - 1)
            def _():
                rows_wait((q - 1, q - 2), sub_idx)

            @pl.when(i == n_q // 2 - 1)
            def _():
                rows_wait((0,), sub_idx)
                cp_wait(sub_idx)

            send(i, q, block, sub_idx)
            carry = step(q, block, sub_idx, 0, scale, shift, carry)
            return step(q - 1, block, sub_idx, 1, scale, shift, carry)

        sums = lax.fori_loop(1, n_q // 2, pair, carry)
        for i in range(rows):
            for p in range(2):
                sums = epilogue(0, block, sub_idx, 1, p, i, sums)
        return sums

    def send(i, q, block, sub_idx):
        buf = 1 - sub_idx
        more = True if sub_idx == 0 else block == 0

        @pl.when((i == 1) & more)
        def _():
            rows_start((n_q,), buf)
            cp_start(buf)

        rows_start((7, 6), buf, (i == 2) & more)
        rows_start((5,), buf, (i == 3) & more)

    def send_rest(block, sub_idx):
        if sub_idx == 0:
            rows_start((4, 3), 1)
        else:
            @pl.when(block == 0)
            def _():
                rows_start((4, 3), 0)

    def block_body(block, _):
        scale, shift = stat_finish(2 * block)
        rows_start((2, 1, 0), 0, block == 1)
        sums = conv_layer(block, 0, scale, shift)
        stat_start(2 * block + 1, *sums)
        send_rest(block, 0)

        @pl.when(block == 0)
        def _():
            for cp in w_copies(2, 0):
                cp.start()

        scale, shift = stat_finish(2 * block + 1)
        rows_start((2, 1, 0), 1)
        sums = conv_layer(block, 1, scale, shift)

        @pl.when(block == 0)
        def _():
            stat_start(2, *sums)
            for cp in w_copies(3, 1):
                cp.start()

        send_rest(block, 1)
        return 0

    lax.fori_loop(0, 2, block_body, 0)
    for layer in range(4):
        for d in range(1, n_dev):
            stat_copy(layer, d).wait_send()


def solution(mesh):
    n_h, n_c = mesh.shape["hp"], mesh.shape["cp"]

    def local_decode(lat, conv_w, conv_b, gamma, beta):
        frames, rows, width, ch = lat.shape
        total = float(frames * n_c * rows * n_h * width * (ch // GROUPS))
        n_q = frames // CHUNK
        cfg = (n_h, n_c, frames, rows, width, ch, total)
        vmem = pl.BlockSpec(memory_space=pltpu.VMEM)
        hbm = pl.BlockSpec(memory_space=pltpu.HBM)
        dma = pltpu.SemaphoreType.DMA
        return pl.pallas_call(
            functools.partial(kernel, cfg),
            out_shape=jax.ShapeDtypeStruct(lat.shape, lat.dtype),
            in_specs=[hbm, hbm, vmem, vmem, vmem],
            out_specs=vmem,
            scratch_shapes=[
                pltpu.VMEM((frames + 2 + CHUNK, rows + 2, width, ch), BF16),
                pltpu.VMEM((frames + 2 + CHUNK, rows + 2, width, ch), BF16),
                pltpu.VMEM((CHUNK + 2, rows + 2, 3, width, ch), BF16),
                pltpu.VMEM((CHUNK + 2, rows + 2, 3, width, ch), BF16),
                pltpu.VMEM((2, 2, 3, 3, ch, ch), BF16),
                pltpu.VMEM((2, 2, 3, 3, ch, ch), BF16),
                pltpu.VMEM((2, 2, 4, 3, ch, ch), BF16),
                pltpu.VMEM((2, 2, 4, 3, ch, ch), BF16),
                pltpu.VMEM((2, 2, rows * width, 2 * ch), F32),
                pltpu.VMEM((2, 2, 2, rows // 2 * width, 2 * ch), F32),
                pltpu.VMEM((4, n_h * n_c, 2, ch), F32),
                dma((n_q,)), dma((2, 6)),
                dma((2, 2, n_q + 1)), dma((2, 2, n_q + 1)), dma((2, 3)), dma((2, 3)),
                dma((4, n_h * n_c)), dma((4, n_h * n_c)),
            ],
            compiler_params=pltpu.CompilerParams(collective_id=0, has_side_effects=True, vmem_limit_bytes=50 * 1024 * 1024),
        )(lat, conv_w, conv_b, gamma, beta)

    spec = P(("dp", "cp"), "hp", None, None)
    return jax.shard_map(local_decode, mesh=mesh, in_specs=(spec, P(), P(), P(), P()), out_specs=spec, check_vma=False)
```
